32 devices in a mesh: grp: 2 (over y), seq: 4 (over z), head: 2 (over x), rep: 2 (over core).
Axes of the slice: x: 2, y: 2, z: 4, core: 2. Of those that a mesh axis runs over, the one named last changes fastest.
Arguments:
- queries: bfloat16 [16, 4096], P(('grp', 'rep'), 'head'), parts along dimension 0, may hold values from -6 to 6
- k_cache: bfloat16 [16, 16, 4096, 128], P(('grp', 'rep'), 'head', 'seq'), parts along dimension 0, may hold values from -6 to 6
- v_cache: bfloat16 [16, 16, 4096, 128], P(('grp', 'rep'), 'head', 'seq'), parts along dimension 0, may hold values from -6 to 6
- page_table: int32 [16, 32], P(('grp', 'rep')), parts along dimension 0, may hold values from 0 to 31, each once within a row
- lengths: int32 [16], P(('grp', 'rep')), parts along dimension 0, may hold values from 512 to 4096
- keep_threshold: int32 [16, 16], P(('grp', 'rep'), 'head'), parts along dimension 0, may hold values from 256 to 8191
Outputs:
- attended: bfloat16 [16, 4096], P(('grp', 'rep'), 'head'), parts along dimension 0
- token_mass: float32 [16, 16, 4096], P(('grp', 'rep'), 'head', 'seq'), parts along dimension 0
- page_keep: float32 [16, 16, 32], P(('grp', 'rep'), 'head', 'seq'), parts along dimension 0
The draws below stay inside these ranges and needn't reach their ends.
There are 2 independent parts, one for each index of `grp`. The reference program is written for one: setup_inputs(seed, part) draws one part's arguments, and reference() takes and returns one part's arrays. A program takes and returns all parts, laid end to end along the dimension named above; each array names one. Nothing has to cross between parts.
Inputs may be any that keep to these rules, and one draw needn't show every extreme that they name: `page_table`: each row names every physical page slot 0 to 31 once.
All inputs are finite; a program needn't handle non-finite values.
Results may differ from the reference program's by a relative error of at most 0.0052.
Values sent between devices are 32-bit elements; how exact they have to be, the bound alone decides.
A program may use at most 64 MiB of HBM per device.

```python
import jax
import jax.numpy as jnp
from jax import lax

QH = 32
KVH = 16
HD = 128
PAGE = 128
BATCH = 8
PAGES = 32
CTX = 4096


def set_ends(drawn, own_key, smallest, top_value):
    index_at = [jax.random.randint(jax.random.fold_in(own_key, axis), (), 0, length) for axis, length in enumerate(drawn.shape)]
    longest = drawn.shape.index(max(drawn.shape))
    neighbour = index_at[:longest] + [(index_at[longest] + 1) % drawn.shape[longest]] + index_at[longest + 1:]
    return drawn.at[tuple(index_at)].set(smallest).at[tuple(neighbour)].set(top_value)


def block_levels(rng, extent, shards, smallest, top_value):
    def one(dim, blocks):
        steps = jax.random.uniform(jax.random.fold_in(jax.random.fold_in(rng, 6), dim), (blocks,), jnp.float32, smallest / len(shards), top_value / len(shards))
        return jnp.repeat(jnp.exp(steps), extent[dim] // blocks).reshape((-1,) + (1,) * (len(extent) - dim - 1))

    gain = one(*shards[0])
    for cut in shards[1:]:
        gain = gain * one(*cut)
    return gain


def centred(own_key, shape, scale, bound, cuts=(), kind=jnp.bfloat16):
    gain = block_levels(own_key, shape, cuts, -0.22, 0.18) if cuts else 1.0
    result = jax.random.normal(own_key, shape, jnp.float32) * scale * gain
    return jnp.minimum(jnp.maximum(result, -bound), bound).astype(kind)


def setup_inputs(seed: int = 0, part: int = 0) -> dict:
    arg_keys = jax.random.split(jax.random.key(seed), 7)
    part_splits = jax.random.split(jax.random.fold_in(arg_keys[6], part), 7)
    return {
        "queries": centred(part_splits[0], (BATCH, QH * HD), 1.0, 6.0, ((0, 2), (1, 2))),
        "k_cache": centred(part_splits[1], (BATCH, KVH, CTX, HD), 1.0, 6.0, ((0, 2), (1, 2), (2, 4))),
        "v_cache": centred(part_splits[2], (BATCH, KVH, CTX, HD), 1.0, 6.0, ((0, 2), (1, 2), (2, 4))),
        "page_table": jax.vmap(lambda own: jax.random.permutation(own, PAGES))(jax.random.split(part_splits[3], BATCH)).reshape((BATCH, PAGES)).astype(jnp.int32),
        "lengths": set_ends(jax.random.randint(part_splits[4], (BATCH,), CTX // 8, CTX + 1), jax.random.fold_in(part_splits[4], 1), CTX // 8, CTX).astype(jnp.int32),
        "keep_threshold": set_ends(jax.random.randint(part_splits[5], (BATCH, KVH), 256, 8192), jax.random.fold_in(part_splits[5], 1), 256, 8191).astype(jnp.int32),
    }


softcap = 50.0
query_scale = 1.0 / 12.0
quanta = 65536.0


def one_request(inputs):
    query_row, keys_all, values_all, table_row, length_one, threshold_row = inputs
    group = QH // KVH
    slots = (table_row[:, None] * PAGE + jnp.arange(PAGE, dtype=jnp.int32)[None, :]).reshape(-1).astype(jnp.int32)
    keys_logical = keys_all[:, slots, :].astype(jnp.float32)
    values_logical = values_all[:, slots, :].astype(jnp.float32)
    grouped = query_row.reshape(KVH, group, HD).astype(jnp.float32)
    logits = jnp.einsum("kgd,ktd->kgt", grouped, keys_logical)
    capped = softcap * jnp.tanh(logits * query_scale / softcap)
    is_live = jnp.arange(CTX, dtype=jnp.int32) < length_one
    weights = jnp.where(is_live[None, None, :], jnp.exp(capped - softcap), jnp.float32(0.0))
    denom = jnp.sum(weights, axis=2)
    numer = jnp.einsum("kgt,ktd->kgd", weights.astype(jnp.bfloat16).astype(jnp.float32), values_logical)
    attended = (numer / denom[:, :, None]).astype(jnp.bfloat16).reshape(QH * HD)
    token_mass = jnp.sum(weights / denom[:, :, None], axis=1)
    page_mass = jnp.sum(token_mass.reshape(KVH, PAGES, PAGE), axis=2)
    page_keep = jnp.minimum(jnp.float32(1.0), quanta * page_mass / threshold_row.astype(jnp.float32)[:, None])
    return attended, token_mass, page_keep


def reference(queries, k_cache, v_cache, page_table, lengths, keep_threshold):
    attended, token_mass, page_keep = lax.map(one_request, (queries, k_cache, v_cache, page_table, lengths, keep_threshold))
    return (attended, token_mass, page_keep)
```

```python
import functools

import jax
import jax.numpy as jnp
from jax import lax
from jax.experimental import pallas as pl
from jax.experimental.pallas import tpu as pltpu
from jax.sharding import PartitionSpec as P

PAGE = 128

softcap = 50.0
query_scale = 1.0 / 12.0
quanta = 65536.0
MESH = pl.DeviceIdType.MESH


def kernel(n, R, KV, G, T, D, *refs):
    (pt_s, len_s, pt_v, q_ref, k_hbm, v_hbm, tm_ref, pm_ref, at_ref) = refs[:9]
    kbuf, vbuf, qbd, maskb, wbuf, dn, nb = refs[9:16]
    gat = refs[16 : 16 + R]
    com = refs[16 + R : 16 + 2 * R]
    ksem, vsem, ds, dr, gs, gr, cs, cr, ns, nr = refs[16 + 2 * R :]
    HG = KV * G
    PL = T // PAGE
    TT = 2 * PAGE
    f32 = jnp.float32
    me = lax.axis_index("seq")

    def k_copy(r):
        return pltpu.make_async_copy(k_hbm.at[r], kbuf.at[r], ksem.at[r])

    def v_copy(r):
        return pltpu.make_async_copy(v_hbm.at[r], vbuf.at[r], vsem.at[r])

    for r in range(R):
        k_copy(r).start()
    for r in range(R):
        v_copy(r).start()

    barrier = pltpu.get_barrier_semaphore()
    for o in range(1, n):
        pl.semaphore_signal(
            barrier, inc=1, device_id={"seq": lax.rem(me + o, n)}, device_id_type=MESH
        )

    row16 = lax.broadcasted_iota(jnp.int32, (HG, 128), 0)
    lane16 = lax.broadcasted_iota(jnp.int32, (HG, 128), 1)
    rowk = lax.rem(row16, KV)

    for r in range(R):
        rows = jnp.concatenate(
            [
                q_ref[r : r + 1, (k * G + g) * D : (k * G + g + 1) * D].astype(f32)
                for g in range(G)
                for k in range(KV)
            ],
            axis=0,
        )
        for k in range(KV):
            qbd[r, :, k * D : (k + 1) * D] = jnp.where(rowk == k, rows, 0.0).astype(jnp.bfloat16)
    pages = pt_v.shape[1]
    slot = me * PL + lax.broadcasted_iota(jnp.int32, (PL, pages), 0)
    jpos = lax.broadcasted_iota(jnp.int32, (PL, pages), 1).astype(f32)
    tok = lax.broadcasted_iota(jnp.int32, (PL, PAGE), 1).astype(f32)
    for r in range(R):
        logical = jnp.sum(
            jnp.where(pt_v[r : r + 1, :] == slot, jpos, 0.0), axis=1, keepdims=True
        )
        limit = len_s[r].astype(f32) - logical * float(PAGE)
        maskb[r] = jnp.where(tok < limit, 1.0, 0.0)

    pl.semaphore_wait(barrier, n - 1)

    def d_copy(r, o):
        return pltpu.make_async_remote_copy(
            src_ref=dn.at[me, r],
            dst_ref=dn.at[me, r],
            send_sem=ds.at[r, o - 1],
            recv_sem=dr.at[r, o - 1],
            device_id={"seq": lax.rem(me + o, n)},
            device_id_type=MESH,
        )

    def scores(r, carry):
        k_copy(r).wait()
        mk = maskb[r]
        total = jnp.zeros((HG, PAGE), f32)
        for t in range(T // TT):
            acc = jnp.zeros((HG, TT), f32)
            for p in range(0, KV, 2):
                kp = jnp.concatenate(
                    [kbuf[r, p, t * TT : (t + 1) * TT, :], kbuf[r, p + 1, t * TT : (t + 1) * TT, :]],
                    axis=1,
                )
                acc += lax.dot_general(
                    qbd[r, :, p * D : (p + 2) * D],
                    kp,
                    (((1,), (1,)), ((), ())),
                    preferred_element_type=f32,
                )
            capped = softcap * jnp.tanh(acc * (query_scale / softcap))
            e = jnp.exp(capped - softcap)
            for c in range(TT // PAGE):
                m = mk[t * (TT // PAGE) + c : t * (TT // PAGE) + c + 1, :]
                w = jnp.where(m > 0.0, e[:, c * PAGE : (c + 1) * PAGE], 0.0)
                lo = t * TT + c * PAGE
                wbuf[r, :, lo : lo + PAGE] = w
                total += w
        col = jnp.sum(total, axis=1, keepdims=True)
        dn[me, r] = jnp.sum(jnp.where(row16 == lane16, col, 0.0), axis=0, keepdims=True)
        for o in range(1, n):
            d_copy(r, o).start()
        return carry

    lax.fori_loop(0, R, scores, 0)

    def denom_of(r):
        tot = dn[0, r]
        for s in range(1, n):
            tot = tot + dn[s, r]
        return jnp.sum(jnp.where(row16 == lane16, tot, 0.0), axis=1, keepdims=True)

    def is_mid(i):
        return jnp.logical_and(i > 0, i < n - 1)

    def g_copy(r, o):
        return pltpu.make_async_remote_copy(
            src_ref=gat[r].at[pl.ds(me * PL, PL)],
            dst_ref=gat[r].at[pl.ds(me * PL, PL)],
            send_sem=gs.at[r, o - 1],
            recv_sem=gr.at[r, o - 1],
            device_id={"seq": lax.rem(me + o, n)},
            device_id_type=MESH,
        )

    def c_copy(r, side):
        return pltpu.make_async_remote_copy(
            src_ref=com[r].at[side],
            dst_ref=gat[r].at[pl.ds(n * PL, PL)],
            send_sem=cs.at[r, side],
            recv_sem=cr.at[r],
            device_id={"seq": (n - 1) * side},
            device_id_type=MESH,
        )

    order = sorted(range(1, n), key=lambda o: -min(o, n - o))
    for r in range(R):
        for o in range(1, n):
            d_copy(r, o).wait_recv()
        den = denom_of(r)
        for c in range(PL):
            w = wbuf[r, :, c * PAGE : (c + 1) * PAGE] / den
            mass = w[0:KV]
            for g in range(1, G):
                mass = mass + w[g * KV : (g + 1) * KV]
            gat[r][me * PL + c] = mass
        for o in order:

            @pl.when(is_mid(lax.rem(me + o, n)))
            def _():
                g_copy(r, o).start()

    def n_copy(r, o):
        return pltpu.make_async_remote_copy(
            src_ref=nb.at[me, r],
            dst_ref=nb.at[me, r],
            send_sem=ns.at[r, o - 1],
            recv_sem=nr.at[r, o - 1],
            device_id={"seq": lax.rem(me + o, n)},
            device_id_type=MESH,
        )

    def mix(r, carry):
        v_copy(r).wait()
        out = jnp.zeros((HG, D), f32)
        for p in range(0, KV, 2):
            acc = jnp.zeros((HG, 2 * D), f32)
            for t in range(T // TT):
                vp = jnp.concatenate(
                    [vbuf[r, p, t * TT : (t + 1) * TT, :], vbuf[r, p + 1, t * TT : (t + 1) * TT, :]],
                    axis=1,
                )
                acc += jnp.dot(
                    wbuf[r, :, t * TT : (t + 1) * TT].astype(jnp.bfloat16),
                    vp,
                    preferred_element_type=f32,
                )
            out = jnp.where(rowk == p, acc[:, :D], out)
            out = jnp.where(rowk == p + 1, acc[:, D:], out)
        nb[me, r] = out
        for o in range(1, n):
            n_copy(r, o).start()
        return carry

    lax.fori_loop(0, R, mix, 0)

    for r in range(R):

        @pl.when(is_mid(me))
        def _():
            for o in range(1, n):
                g_copy(r, o).wait_recv()

        for side in (0, 1):

            @pl.when(me == (1 if side == 0 else n - 2))
            def _():
                for m in range(PL):
                    com[r][side, m] = gat[r][pt_s[r, side * (n - 1) * PL + m]]
                c_copy(r, side).start()

    lane_pl = lax.broadcasted_iota(jnp.int32, (KV, PAGE), 1)
    at_end = jnp.logical_not(is_mid(me))
    for r in range(R):

        @pl.when(at_end)
        def _():
            c_copy(r, 0).wait_recv()

        sums = jnp.zeros((KV, PAGE), f32)
        for m in range(PL):
            p = pt_s[r, me * PL + m]
            away = jnp.logical_or(p < me * PL, p >= (me + 1) * PL)
            idx = jnp.where(jnp.logical_and(at_end, away), n * PL + m, p)
            page = gat[r][idx]
            tm_ref[r, :, m * PAGE : (m + 1) * PAGE] = page
            sums = jnp.where(lane_pl == m, jnp.sum(page, axis=1, keepdims=True), sums)
        pm_ref[r] = sums[:, :PL]

    for r in range(R):
        for o in range(1, n):
            n_copy(r, o).wait_recv()
        tot = nb[0, r]
        for s in range(1, n):
            tot = tot + nb[s, r]
        at_ref[r] = tot / denom_of(r)

    for r in range(R):
        for o in range(1, n):
            d_copy(r, o).wait_send()
            n_copy(r, o).wait_send()

            @pl.when(is_mid(lax.rem(me + o, n)))
            def _():
                g_copy(r, o).wait_send()

        for side in (0, 1):

            @pl.when(me == (1 if side == 0 else n - 2))
            def _():
                c_copy(r, side).wait_send()


def shards(n, queries, k_cache, v_cache, page_table, lengths, keep_threshold):
    R, KV, T, D = k_cache.shape
    G = queries.shape[1] // D // KV
    HG = KV * G
    PL = T // PAGE
    f32 = jnp.float32
    vmem = pl.BlockSpec(memory_space=pltpu.VMEM)
    smem = pl.BlockSpec(memory_space=pltpu.SMEM)
    hbm = pl.BlockSpec(memory_space=pl.ANY)
    dma = pltpu.SemaphoreType.DMA
    owned, mass, att = pl.pallas_call(
        functools.partial(kernel, n, R, KV, G, T, D),
        out_shape=(
            jax.ShapeDtypeStruct((R, KV, T), f32),
            jax.ShapeDtypeStruct((R, KV, PL), f32),
            jax.ShapeDtypeStruct((R, HG, D), f32),
        ),
        in_specs=[smem, smem, vmem, vmem, hbm, hbm],
        out_specs=(vmem, vmem, vmem),
        scratch_shapes=[
            pltpu.VMEM((R, KV, T, D), jnp.bfloat16),
            pltpu.VMEM((R, KV, T, D), jnp.bfloat16),
            pltpu.VMEM((R, HG, KV * D), jnp.bfloat16),
            pltpu.VMEM((R, PL, PAGE), f32),
            pltpu.VMEM((R, HG, T), f32),
            pltpu.VMEM((n, R, 1, 128), f32),
            pltpu.VMEM((n, R, HG, D), f32),
        ]
        + [pltpu.VMEM(((n + 1) * PL, KV, PAGE), f32)] * R
        + [pltpu.VMEM((2, PL, KV, PAGE), f32)] * R
        + [
            dma((R,)),
            dma((R,)),
            dma((R, n - 1)),
            dma((R, n - 1)),
            dma((R, n - 1)),
            dma((R, n - 1)),
            dma((R, 2)),
            dma((R,)),
            dma((R, n - 1)),
            dma((R, n - 1)),
        ],
        compiler_params=pltpu.CompilerParams(collective_id=0, has_side_effects=True),
    )(page_table, lengths, page_table, queries, k_cache, v_cache)
    attended = (
        att.reshape(R, G, KV, D).transpose(0, 2, 1, 3).reshape(R, HG * D).astype(jnp.bfloat16)
    )
    page_keep = jnp.minimum(1.0, quanta * mass / keep_threshold.astype(f32)[:, :, None])
    return attended, owned, page_keep


def solution(mesh):
    placed = (
        P(("grp", "rep"), "head"),
        P(("grp", "rep"), "head", "seq", None),
        P(("grp", "rep"), "head", "seq", None),
        P(("grp", "rep"), None),
        P(("grp", "rep")),
        P(("grp", "rep"), "head"),
    )
    return jax.shard_map(
        functools.partial(shards, mesh.shape["seq"]),
        mesh=mesh,
        in_specs=placed,
        out_specs=(
            P(("grp", "rep"), "head"),
            P(("grp", "rep"), "head", "seq"),
            P(("grp", "rep"), "head", "seq"),
        ),
        check_vma=False,
    )
```

```python
import functools

import jax
import jax.numpy as jnp
from jax import lax
from jax.experimental import pallas as pl
from jax.experimental.pallas import tpu as pltpu
from jax.sharding import PartitionSpec as P

PAGE = 128

softcap = 50.0
query_scale = 1.0 / 12.0
quanta = 65536.0
MESH = pl.DeviceIdType.MESH


def kernel(n, R, KV, G, T, D, *refs):
    (pt_s, len_s, pt_v, q_ref, k_hbm, v_hbm, tm_ref, at_ref) = refs[:8]
    kbuf, vbuf, qbd, maskb, wbuf, dn, nb = refs[8:15]
    gat = refs[15 : 15 + R]
    com = refs[15 + R : 15 + 2 * R]
    ksem, vsem, ds, dr, gs, gr, cs, cr, ns, nr = refs[15 + 2 * R :]
    HG = KV * G
    PL = T // PAGE
    TT = 2 * PAGE
    f32 = jnp.float32
    me = lax.axis_index("seq")

    def k_copy(r):
        return pltpu.make_async_copy(k_hbm.at[r], kbuf.at[r], ksem.at[r])

    def v_copy(r):
        return pltpu.make_async_copy(v_hbm.at[r], vbuf.at[r], vsem.at[r])

    for r in range(R):
        k_copy(r).start()
    barrier = pltpu.get_barrier_semaphore()
    for o in range(1, n):
        pl.semaphore_signal(
            barrier, inc=1, device_id={"seq": lax.rem(me + o, n)}, device_id_type=MESH
        )

    row16 = lax.broadcasted_iota(jnp.int32, (HG, 128), 0)
    lane16 = lax.broadcasted_iota(jnp.int32, (HG, 128), 1)
    rowk = lax.rem(row16, KV)

    for r in range(R):
        rows = jnp.concatenate(
            [
                q_ref[r : r + 1, (k * G + g) * D : (k * G + g + 1) * D].astype(f32)
                for g in range(G)
                for k in range(KV)
            ],
            axis=0,
        )
        for k in range(KV):
            qbd[r, :, k * D : (k + 1) * D] = jnp.where(rowk == k, rows, 0.0).astype(jnp.bfloat16)
    pages = pt_v.shape[1]
    slot = me * PL + lax.broadcasted_iota(jnp.int32, (PL, pages), 0)
    jpos = lax.broadcasted_iota(jnp.int32, (PL, pages), 1).astype(f32)
    tok = lax.broadcasted_iota(jnp.int32, (PL, PAGE), 1).astype(f32)
    for r in range(R):
        logical = jnp.sum(
            jnp.where(pt_v[r : r + 1, :] == slot, jpos, 0.0), axis=1, keepdims=True
        )
        limit = len_s[r].astype(f32) - logical * float(PAGE)
        maskb[r] = jnp.where(tok < limit, 1.0, 0.0)

    pl.semaphore_wait(barrier, n - 1)

    def d_copy(r, o):
        return pltpu.make_async_remote_copy(
            src_ref=dn.at[me, r],
            dst_ref=dn.at[me, r],
            send_sem=ds.at[r, o - 1],
            recv_sem=dr.at[r, o - 1],
            device_id={"seq": lax.rem(me + o, n)},
            device_id_type=MESH,
        )

    def scores(r, carry):
        k_copy(r).wait()
        v_copy(r).start()
        mk = maskb[r]
        total = jnp.zeros((HG, PAGE), f32)
        for t in range(T // TT):
            acc = jnp.zeros((HG, TT), f32)
            for p in range(0, KV, 2):
                kp = jnp.concatenate(
                    [kbuf[r, p, t * TT : (t + 1) * TT, :], kbuf[r, p + 1, t * TT : (t + 1) * TT, :]],
                    axis=1,
                )
                acc += lax.dot_general(
                    qbd[r, :, p * D : (p + 2) * D],
                    kp,
                    (((1,), (1,)), ((), ())),
                    preferred_element_type=f32,
                )
            capped = softcap * jnp.tanh(acc * (query_scale / softcap))
            e = jnp.exp(capped - softcap)
            for c in range(TT // PAGE):
                m = mk[t * (TT // PAGE) + c : t * (TT // PAGE) + c + 1, :]
                w = jnp.where(m > 0.0, e[:, c * PAGE : (c + 1) * PAGE], 0.0)
                lo = t * TT + c * PAGE
                wbuf[r, :, lo : lo + PAGE] = w
                total += w
        col = jnp.sum(total, axis=1, keepdims=True)
        dn[me, r] = jnp.sum(jnp.where(row16 == lane16, col, 0.0), axis=0, keepdims=True)
        for o in range(1, n):
            d_copy(r, o).start()
        return carry

    lax.fori_loop(0, R, scores, 0)

    def denom_of(r):
        tot = dn[0, r]
        for s in range(1, n):
            tot = tot + dn[s, r]
        return jnp.sum(jnp.where(row16 == lane16, tot, 0.0), axis=1, keepdims=True)

    def is_mid(i):
        return jnp.logical_and(i > 0, i < n - 1)

    def g_copy(r, o):
        return pltpu.make_async_remote_copy(
            src_ref=gat[r].at[pl.ds(me * PL, PL)],
            dst_ref=gat[r].at[pl.ds(me * PL, PL)],
            send_sem=gs.at[r, o - 1],
            recv_sem=gr.at[r, o - 1],
            device_id={"seq": lax.rem(me + o, n)},
            device_id_type=MESH,
        )

    def c_copy(r, side):
        return pltpu.make_async_remote_copy(
            src_ref=com[r].at[side],
            dst_ref=gat[r].at[pl.ds(n * PL, PL)],
            send_sem=cs.at[r, side],
            recv_sem=cr.at[r],
            device_id={"seq": (n - 1) * side},
            device_id_type=MESH,
        )

    def n_copy(r, o):
        return pltpu.make_async_remote_copy(
            src_ref=nb.at[me, r],
            dst_ref=nb.at[me, r],
            send_sem=ns.at[r, o - 1],
            recv_sem=nr.at[r, o - 1],
            device_id={"seq": lax.rem(me + o, n)},
            device_id_type=MESH,
        )

    def mix(r, carry):
        v_copy(r).wait()
        out = jnp.zeros((HG, D), f32)
        for p in range(0, KV, 2):
            acc = jnp.zeros((HG, 2 * D), f32)
            for t in range(T // TT):
                vp = jnp.concatenate(
                    [vbuf[r, p, t * TT : (t + 1) * TT, :], vbuf[r, p + 1, t * TT : (t + 1) * TT, :]],
                    axis=1,
                )
                acc += jnp.dot(
                    wbuf[r, :, t * TT : (t + 1) * TT].astype(jnp.bfloat16),
                    vp,
                    preferred_element_type=f32,
                )
            out = jnp.where(rowk == p, acc[:, :D], out)
            out = jnp.where(rowk == p + 1, acc[:, D:], out)
        nb[me, r] = out
        for o in range(1, n):
            n_copy(r, o).start()
        return carry

    order = sorted(range(1, n), key=lambda o: -min(o, n - o))
    def spread(r):
        for o in range(1, n):
            d_copy(r, o).wait_recv()
        den = denom_of(r)
        for c in range(PL):
            w = wbuf[r, :, c * PAGE : (c + 1) * PAGE] / den
            mass = w[0:KV]
            for g in range(1, G):
                mass = mass + w[g * KV : (g + 1) * KV]
            gat[r][me * PL + c] = mass
        for o in order:

            @pl.when(is_mid(lax.rem(me + o, n)))
            def _():
                g_copy(r, o).start()

    for r in range(R):
        spread(r)
        lax.fori_loop(r, r + 1, mix, 0)

    for r in range(R):

        @pl.when(is_mid(me))
        def _():
            for o in range(1, n):
                g_copy(r, o).wait_recv()

        for side in (0, 1):

            @pl.when(me == (1 if side == 0 else n - 2))
            def _():
                for m in range(PL):
                    com[r][side, m] = gat[r][pt_s[r, side * (n - 1) * PL + m]]
                c_copy(r, side).start()

    at_end = jnp.logical_not(is_mid(me))
    for r in range(R):

        @pl.when(at_end)
        def _():
            c_copy(r, 0).wait_recv()

        for m in range(PL):
            p = pt_s[r, me * PL + m]
            away = jnp.logical_or(p < me * PL, p >= (me + 1) * PL)
            idx = jnp.where(jnp.logical_and(at_end, away), n * PL + m, p)
            page = gat[r][idx]
            tm_ref[r, :, m * PAGE : (m + 1) * PAGE] = page

    for r in range(R):
        for o in range(1, n):
            n_copy(r, o).wait_recv()
        tot = nb[0, r]
        for s in range(1, n):
            tot = tot + nb[s, r]
        at_ref[r] = tot / denom_of(r)

    for r in range(R):
        for o in range(1, n):
            d_copy(r, o).wait_send()
            n_copy(r, o).wait_send()

            @pl.when(is_mid(lax.rem(me + o, n)))
            def _():
                g_copy(r, o).wait_send()

        for side in (0, 1):

            @pl.when(me == (1 if side == 0 else n - 2))
            def _():
                c_copy(r, side).wait_send()


def finish(R, KV, G, T, D, own_ref, att_ref, keep_ref, at_ref, tm_ref, pk_ref, sem):
    PL = T // PAGE
    f32 = jnp.float32
    out = pltpu.make_async_copy(own_ref, tm_ref, sem)
    out.start()
    for k in range(KV):
        for g in range(G):
            h = k * G + g
            at_ref[:, h * D : (h + 1) * D] = att_ref[:, g * KV + k, :].astype(jnp.bfloat16)
    lane = lax.broadcasted_iota(jnp.int32, (KV, PAGE), 1)
    diag = lax.broadcasted_iota(jnp.int32, (KV, KV), 0) == lax.broadcasted_iota(
        jnp.int32, (KV, KV), 1
    )
    for r in range(R):
        sums = jnp.zeros((KV, PAGE), f32)
        for m in range(PL):
            page = own_ref[r, :, m * PAGE : (m + 1) * PAGE]
            sums = jnp.where(lane == m, jnp.sum(page, axis=1, keepdims=True), sums)
        row = keep_ref[r : r + 1, :].astype(f32)
        keep = jnp.sum(jnp.where(diag, row, 0.0), axis=1, keepdims=True)
        pk_ref[r] = jnp.minimum(1.0, quanta * sums / keep)[:, :PL]
    out.wait()


def shards(n, queries, k_cache, v_cache, page_table, lengths, keep_threshold):
    R, KV, T, D = k_cache.shape
    G = queries.shape[1] // D // KV
    HG = KV * G
    PL = T // PAGE
    f32 = jnp.float32
    vmem = pl.BlockSpec(memory_space=pltpu.VMEM)
    smem = pl.BlockSpec(memory_space=pltpu.SMEM)
    hbm = pl.BlockSpec(memory_space=pl.ANY)
    dma = pltpu.SemaphoreType.DMA
    owned, att = pl.pallas_call(
        functools.partial(kernel, n, R, KV, G, T, D),
        out_shape=(
            pltpu.VMEM((R, KV, T), f32),
            pltpu.VMEM((R, HG, D), f32),
        ),
        in_specs=[smem, smem, vmem, vmem, hbm, hbm],
        out_specs=(vmem, vmem),
        scratch_shapes=[
            pltpu.VMEM((R, KV, T, D), jnp.bfloat16),
            pltpu.VMEM((R, KV, T, D), jnp.bfloat16),
            pltpu.VMEM((R, HG, KV * D), jnp.bfloat16),
            pltpu.VMEM((R, PL, PAGE), f32),
            pltpu.VMEM((R, HG, T), f32),
            pltpu.VMEM((n, R, 1, 128), f32),
            pltpu.VMEM((n, R, HG, D), f32),
        ]
        + [pltpu.VMEM(((n + 1) * PL, KV, PAGE), f32)] * R
        + [pltpu.VMEM((2, PL, KV, PAGE), f32)] * R
        + [
            dma((R,)),
            dma((R,)),
            dma((R, n - 1)),
            dma((R, n - 1)),
            dma((R, n - 1)),
            dma((R, n - 1)),
            dma((R, 2)),
            dma((R,)),
            dma((R, n - 1)),
            dma((R, n - 1)),
        ],
        compiler_params=pltpu.CompilerParams(collective_id=0, has_side_effects=True),
    )(page_table, lengths, page_table, queries, k_cache, v_cache)
    owned = pltpu.with_memory_space_constraint(owned, pltpu.VMEM)
    att = pltpu.with_memory_space_constraint(att, pltpu.VMEM)
    return pl.pallas_call(
        functools.partial(finish, R, KV, G, T, D),
        out_shape=(
            jax.ShapeDtypeStruct((R, HG * D), jnp.bfloat16),
            jax.ShapeDtypeStruct((R, KV, T), f32),
            jax.ShapeDtypeStruct((R, KV, PL), f32),
        ),
        in_specs=[vmem, vmem, vmem],
        out_specs=(vmem, hbm, vmem),
        scratch_shapes=[dma],
    )(owned, att, keep_threshold)


def solution(mesh):
    placed = (
        P(("grp", "rep"), "head"),
        P(("grp", "rep"), "head", "seq", None),
        P(("grp", "rep"), "head", "seq", None),
        P(("grp", "rep"), None),
        P(("grp", "rep")),
        P(("grp", "rep"), "head"),
    )
    return jax.shard_map(
        functools.partial(shards, mesh.shape["seq"]),
        mesh=mesh,
        in_specs=placed,
        out_specs=(
            P(("grp", "rep"), "head"),
            P(("grp", "rep"), "head", "seq"),
            P(("grp", "rep"), "head", "seq"),
        ),
        check_vma=False,
    )
```

```python
import functools

import jax
import jax.numpy as jnp
from jax import lax
from jax.experimental import pallas as pl
from jax.experimental.pallas import tpu as pltpu
from jax.sharding import PartitionSpec as P

PAGE = 128

softcap = 50.0
query_scale = 1.0 / 12.0
quanta = 65536.0
MESH = pl.DeviceIdType.MESH


def kernel(n, R, KV, G, T, D, *refs):
    (pt_s, len_s, pt_v, q_ref, k_hbm, v_hbm, tm_ref, at_ref) = refs[:8]
    kbuf, vbuf, qbd, maskb, wbuf, dn, nb, rb, ab, denb = refs[8:18]
    gat = refs[18 : 18 + R]
    com = refs[18 + R : 18 + 2 * R]
    ksem, vsem, ds, dr, gs, gr, cs, cr, ns, nr, fs, fr = refs[18 + 2 * R :]
    HG = KV * G
    rows_of = R * HG // n
    parts = HG // rows_of
    PL = T // PAGE
    TT = 2 * PAGE
    f32 = jnp.float32
    me = lax.axis_index("seq")

    def k_copy(r):
        return pltpu.make_async_copy(k_hbm.at[r], kbuf.at[r], ksem.at[r])

    def v_copy(r):
        return pltpu.make_async_copy(v_hbm.at[r], vbuf.at[r], vsem.at[r])

    for r in range(R):
        k_copy(r).start()
    barrier = pltpu.get_barrier_semaphore()
    for o in range(1, n):
        pl.semaphore_signal(
            barrier, inc=1, device_id={"seq": lax.rem(me + o, n)}, device_id_type=MESH
        )

    row16 = lax.broadcasted_iota(jnp.int32, (HG, 128), 0)
    lane16 = lax.broadcasted_iota(jnp.int32, (HG, 128), 1)
    rowk = lax.rem(row16, KV)

    for r in range(R):
        rows = jnp.concatenate(
            [
                q_ref[r : r + 1, (k * G + g) * D : (k * G + g + 1) * D].astype(f32)
                for g in range(G)
                for k in range(KV)
            ],
            axis=0,
        )
        for k in range(KV):
            qbd[r, :, k * D : (k + 1) * D] = jnp.where(rowk == k, rows, 0.0).astype(jnp.bfloat16)
    pages = pt_v.shape[1]
    slot = me * PL + lax.broadcasted_iota(jnp.int32, (PL, pages), 0)
    jpos = lax.broadcasted_iota(jnp.int32, (PL, pages), 1).astype(f32)
    tok = lax.broadcasted_iota(jnp.int32, (PL, PAGE), 1).astype(f32)
    for r in range(R):
        logical = jnp.sum(
            jnp.where(pt_v[r : r + 1, :] == slot, jpos, 0.0), axis=1, keepdims=True
        )
        limit = len_s[r].astype(f32) - logical * float(PAGE)
        maskb[r] = jnp.where(tok < limit, 1.0, 0.0)

    pl.semaphore_wait(barrier, n - 1)

    def d_copy(r, o):
        return pltpu.make_async_remote_copy(
            src_ref=dn.at[me, r],
            dst_ref=dn.at[me, r],
            send_sem=ds.at[r, o - 1],
            recv_sem=dr.at[r, o - 1],
            device_id={"seq": lax.rem(me + o, n)},
            device_id_type=MESH,
        )

    def scores(r, carry):
        k_copy(r).wait()
        v_copy(r).start()
        mk = maskb[r]
        total = jnp.zeros((HG, PAGE), f32)
        for t in range(T // TT):
            acc = jnp.zeros((HG, TT), f32)
            for p in range(0, KV, 2):
                kp = jnp.concatenate(
                    [kbuf[r, p, t * TT : (t + 1) * TT, :], kbuf[r, p + 1, t * TT : (t + 1) * TT, :]],
                    axis=1,
                )
                acc += lax.dot_general(
                    qbd[r, :, p * D : (p + 2) * D],
                    kp,
                    (((1,), (1,)), ((), ())),
                    preferred_element_type=f32,
                )
            capped = softcap * jnp.tanh(acc * (query_scale / softcap))
            e = jnp.exp(capped - softcap)
            for c in range(TT // PAGE):
                m = mk[t * (TT // PAGE) + c : t * (TT // PAGE) + c + 1, :]
                w = jnp.where(m > 0.0, e[:, c * PAGE : (c + 1) * PAGE], 0.0)
                lo = t * TT + c * PAGE
                wbuf[r, :, lo : lo + PAGE] = w
                total += w
        col = jnp.sum(total, axis=1, keepdims=True)
        dn[me, r] = jnp.sum(jnp.where(row16 == lane16, col, 0.0), axis=0, keepdims=True)
        for o in range(1, n):
            d_copy(r, o).start()
        return carry

    lax.fori_loop(0, R, scores, 0)

    def denom_of(r):
        tot = dn[0, r]
        for s in range(1, n):
            tot = tot + dn[s, r]
        return jnp.sum(jnp.where(row16 == lane16, tot, 0.0), axis=1, keepdims=True)

    def is_mid(i):
        return jnp.logical_and(i > 0, i < n - 1)

    def g_copy(r, o):
        return pltpu.make_async_remote_copy(
            src_ref=gat[r].at[pl.ds(me * PL, PL)],
            dst_ref=gat[r].at[pl.ds(me * PL, PL)],
            send_sem=gs.at[r, o - 1],
            recv_sem=gr.at[r, o - 1],
            device_id={"seq": lax.rem(me + o, n)},
            device_id_type=MESH,
        )

    def c_copy(r, side):
        return pltpu.make_async_remote_copy(
            src_ref=com[r].at[side],
            dst_ref=gat[r].at[pl.ds(n * PL, PL)],
            send_sem=cs.at[r, side],
            recv_sem=cr.at[r],
            device_id={"seq": (n - 1) * side},
            device_id_type=MESH,
        )

    def n_copy(p, source):
        return pltpu.make_async_remote_copy(
            src_ref=nb.at[p],
            dst_ref=rb.at[source],
            send_sem=ns.at[p],
            recv_sem=nr.at[source],
            device_id={"seq": p},
            device_id_type=MESH,
        )

    def f_copy(o):
        return pltpu.make_async_remote_copy(
            src_ref=ab.at[me],
            dst_ref=ab.at[me],
            send_sem=fs.at[o - 1],
            recv_sem=fr.at[o - 1],
            device_id={"seq": lax.rem(me + o, n)},
            device_id_type=MESH,
        )

    def mix(r, carry):
        v_copy(r).wait()
        out = jnp.zeros((HG, D), f32)
        for p in range(0, KV, 2):
            acc = jnp.zeros((HG, 2 * D), f32)
            for t in range(T // TT):
                vp = jnp.concatenate(
                    [vbuf[r, p, t * TT : (t + 1) * TT, :], vbuf[r, p + 1, t * TT : (t + 1) * TT, :]],
                    axis=1,
                )
                acc += jnp.dot(
                    wbuf[r, :, t * TT : (t + 1) * TT].astype(jnp.bfloat16),
                    vp,
                    preferred_element_type=f32,
                )
            out = jnp.where(rowk == p, acc[:, :D], out)
            out = jnp.where(rowk == p + 1, acc[:, D:], out)
        for j in range(parts):
            nb[r * parts + j] = out[j * rows_of : (j + 1) * rows_of]
        for j in range(parts):
            dest = r * parts + j

            @pl.when(dest != me)
            def _():
                n_copy(dest, me).start()

        return carry

    order = sorted(range(1, n), key=lambda o: -min(o, n - o))
    def spread(r):
        for o in range(1, n):
            d_copy(r, o).wait_recv()
        den = denom_of(r)
        wide = jnp.broadcast_to(den, (HG, D))
        for j in range(parts):
            denb[r * parts + j] = wide[j * rows_of : (j + 1) * rows_of]
        for c in range(PL):
            w = wbuf[r, :, c * PAGE : (c + 1) * PAGE] / den
            mass = w[0:KV]
            for g in range(1, G):
                mass = mass + w[g * KV : (g + 1) * KV]
            gat[r][me * PL + c] = mass
        for o in order:

            @pl.when(is_mid(lax.rem(me + o, n)))
            def _():
                g_copy(r, o).start()

    for r in range(R):
        spread(r)
    lax.fori_loop(0, R, mix, 0)

    def combine():
        rb[me] = nb[me]
        for s in range(n):

            @pl.when(me != s)
            def _():
                n_copy(me, s).wait_recv()

        tot = rb[0]
        for s in range(1, n):
            tot = tot + rb[s]
        ab[me] = tot / denb[me]
        for o in range(1, n):
            f_copy(o).start()

    def compact(r):

        @pl.when(is_mid(me))
        def _():
            for o in range(1, n):
                g_copy(r, o).wait_recv()

        for side in (0, 1):

            @pl.when(me == (1 if side == 0 else n - 2))
            def _():
                for m in range(PL):
                    com[r][side, m] = gat[r][pt_s[r, side * (n - 1) * PL + m]]
                c_copy(r, side).start()

    for r in range(R // 2):
        compact(r)
    combine()
    for r in range(R // 2, R):
        compact(r)

    at_end = jnp.logical_not(is_mid(me))
    for r in range(R):

        @pl.when(at_end)
        def _():
            c_copy(r, 0).wait_recv()

        for m in range(PL):
            p = pt_s[r, me * PL + m]
            away = jnp.logical_or(p < me * PL, p >= (me + 1) * PL)
            idx = jnp.where(jnp.logical_and(at_end, away), n * PL + m, p)
            page = gat[r][idx]
            tm_ref[r, :, m * PAGE : (m + 1) * PAGE] = page

    for o in range(1, n):
        f_copy(o).wait_recv()
    for r in range(R):
        for j in range(parts):
            at_ref[r, j * rows_of : (j + 1) * rows_of] = ab[r * parts + j]

    for p in range(n):

        @pl.when(me != p)
        def _():
            n_copy(p, me).wait_send()

    for o in range(1, n):
        f_copy(o).wait_send()
    for r in range(R):
        for o in range(1, n):
            d_copy(r, o).wait_send()

            @pl.when(is_mid(lax.rem(me + o, n)))
            def _():
                g_copy(r, o).wait_send()

        for side in (0, 1):

            @pl.when(me == (1 if side == 0 else n - 2))
            def _():
                c_copy(r, side).wait_send()


def finish(R, KV, G, T, D, own_ref, att_ref, keep_ref, at_ref, tm_ref, pk_ref, sem):
    PL = T // PAGE
    f32 = jnp.float32
    out = pltpu.make_async_copy(own_ref, tm_ref, sem)
    out.start()
    for k in range(KV):
        for g in range(G):
            h = k * G + g
            at_ref[:, h * D : (h + 1) * D] = att_ref[:, g * KV + k, :].astype(jnp.bfloat16)
    lane = lax.broadcasted_iota(jnp.int32, (KV, PAGE), 1)
    diag = lax.broadcasted_iota(jnp.int32, (KV, KV), 0) == lax.broadcasted_iota(
        jnp.int32, (KV, KV), 1
    )
    for r in range(R):
        sums = jnp.zeros((KV, PAGE), f32)
        for m in range(PL):
            page = own_ref[r, :, m * PAGE : (m + 1) * PAGE]
            sums = jnp.where(lane == m, jnp.sum(page, axis=1, keepdims=True), sums)
        row = keep_ref[r : r + 1, :].astype(f32)
        keep = jnp.sum(jnp.where(diag, row, 0.0), axis=1, keepdims=True)
        pk_ref[r] = jnp.minimum(1.0, quanta * sums / keep)[:, :PL]
    out.wait()


def shards(n, queries, k_cache, v_cache, page_table, lengths, keep_threshold):
    R, KV, T, D = k_cache.shape
    G = queries.shape[1] // D // KV
    HG = KV * G
    PL = T // PAGE
    f32 = jnp.float32
    vmem = pl.BlockSpec(memory_space=pltpu.VMEM)
    smem = pl.BlockSpec(memory_space=pltpu.SMEM)
    hbm = pl.BlockSpec(memory_space=pl.ANY)
    dma = pltpu.SemaphoreType.DMA
    owned, att = pl.pallas_call(
        functools.partial(kernel, n, R, KV, G, T, D),
        out_shape=(
            pltpu.VMEM((R, KV, T), f32),
            pltpu.VMEM((R, HG, D), f32),
        ),
        in_specs=[smem, smem, vmem, vmem, hbm, hbm],
        out_specs=(vmem, vmem),
        scratch_shapes=[
            pltpu.VMEM((R, KV, T, D), jnp.bfloat16),
            pltpu.VMEM((R, KV, T, D), jnp.bfloat16),
            pltpu.VMEM((R, HG, KV * D), jnp.bfloat16),
            pltpu.VMEM((R, PL, PAGE), f32),
            pltpu.VMEM((R, HG, T), f32),
            pltpu.VMEM((n, R, 1, 128), f32),
            pltpu.VMEM((n, R * HG // n, D), f32),
            pltpu.VMEM((n, R * HG // n, D), f32),
            pltpu.VMEM((n, R * HG // n, D), f32),
            pltpu.VMEM((n, R * HG // n, D), f32),
        ]
        + [pltpu.VMEM(((n + 1) * PL, KV, PAGE), f32)] * R
        + [pltpu.VMEM((2, PL, KV, PAGE), f32)] * R
        + [
            dma((R,)),
            dma((R,)),
            dma((R, n - 1)),
            dma((R, n - 1)),
            dma((R, n - 1)),
            dma((R, n - 1)),
            dma((R, 2)),
            dma((R,)),
            dma((n,)),
            dma((n,)),
            dma((n - 1,)),
            dma((n - 1,)),
        ],
        compiler_params=pltpu.CompilerParams(collective_id=0, has_side_effects=True),
    )(page_table, lengths, page_table, queries, k_cache, v_cache)
    owned = pltpu.with_memory_space_constraint(owned, pltpu.VMEM)
    att = pltpu.with_memory_space_constraint(att, pltpu.VMEM)
    return pl.pallas_call(
        functools.partial(finish, R, KV, G, T, D),
        out_shape=(
            jax.ShapeDtypeStruct((R, HG * D), jnp.bfloat16),
            jax.ShapeDtypeStruct((R, KV, T), f32),
            jax.ShapeDtypeStruct((R, KV, PL), f32),
        ),
        in_specs=[vmem, vmem, vmem],
        out_specs=(vmem, hbm, vmem),
        scratch_shapes=[dma],
    )(owned, att, keep_threshold)


def solution(mesh):
    placed = (
        P(("grp", "rep"), "head"),
        P(("grp", "rep"), "head", "seq", None),
        P(("grp", "rep"), "head", "seq", None),
        P(("grp", "rep"), None),
        P(("grp", "rep")),
        P(("grp", "rep"), "head"),
    )
    return jax.shard_map(
        functools.partial(shards, mesh.shape["seq"]),
        mesh=mesh,
        in_specs=placed,
        out_specs=(
            P(("grp", "rep"), "head"),
            P(("grp", "rep"), "head", "seq"),
            P(("grp", "rep"), "head", "seq"),
        ),
        check_vma=False,
    )
```
